32 devices in a mesh: panel: 8 (over z, core), rhs: 4 (over y, x).
Axes of the slice: x: 2, y: 2, z: 4, core: 2. Of those that a mesh axis runs over, the one named last changes fastest.
Arguments:
- pivot_rhs: float32 [2, 2048, 512], P(None, 'panel', 'rhs'), may hold values from -6 to 6
- update_rhs: float32 [4096, 512], P('panel', 'rhs'), may hold values from -6 to 6
- parent_rhs: float32 [4096, 512], P('panel', 'rhs'), may hold values from -6 to 6
- lower_pivot: bfloat16 [2, 2048, 2048], P(None, 'panel', 'rhs'), may hold values from -1 to 1.4, as said below
- lower_update: bfloat16 [4096, 2048], P('panel', 'rhs'), may hold values from -0.125 to 0.125
- parent_lower: bfloat16 [4096, 4096], P('panel', 'rhs'), may hold values from -1 to 1.4, as said below
- parent_upper: bfloat16 [4096, 4096], P('panel', 'rhs'), may hold values from -1 to 1.4, as said below
- upper_pivot: bfloat16 [2, 2048, 2048], P(None, 'panel', 'rhs'), may hold values from -1 to 1.4, as said below
- upper_update: bfloat16 [2, 2048, 2048], P(None, 'panel', 'rhs'), may hold values from -0.125 to 0.125
- maps: int32 [4096], replicated, may hold values from 0 to 4095, as said below
Outputs:
- parent_solution: float32 [4096, 512], P('panel', 'rhs')
- child_solution: float32 [2, 2048, 512], P(None, 'panel', 'rhs')
The draws below stay inside these ranges and needn't reach their ends.
Inputs may be any that keep to these rules, and one draw needn't show every extreme that they name: `maps`: for each child k, entry k * 2048 + i is 2 * i + b with b equal to 0 or 1; both values of b occur for each child in every draw. `lower_pivot`: each block is lower triangular, diagonal 0.6 to 1.4. `upper_pivot`: each block is upper triangular, diagonal 0.6 to 1.4. `parent_lower`: lower triangular, diagonal 0.6 to 1.4. `parent_upper`: upper triangular, diagonal 0.6 to 1.4.
All inputs are finite; a program needn't handle non-finite values.
Results may differ from the reference program's by a relative error of at most 0.0054.
Values may be sent and summed in bfloat16 or wider, within the bound.
A program may use at most 64 MiB of HBM per device.

```python
import math
import jax
import jax.numpy as jnp
from jax import lax

F = 4096
KC = 2048
FU = 2048
RHS = 512


def triangle(random_key, block_count, matrix_order, lower_side):
    shape_full = (block_count, matrix_order, matrix_order)
    noise = jax.random.normal(random_key, shape_full, jnp.float32)
    noise = noise / math.sqrt(matrix_order)
    row_ids = lax.broadcasted_iota(jnp.int32, (matrix_order, matrix_order), 0)
    col_ids = lax.broadcasted_iota(jnp.int32, (matrix_order, matrix_order), 1)
    if lower_side:
        keeper = row_ids > col_ids
    else:
        keeper = row_ids < col_ids
    diagonal_scale = jax.random.uniform(jax.random.fold_in(random_key, 7), (block_count, matrix_order, 1), jnp.float32, 0.6, 1.4)
    identity = jnp.where(row_ids == col_ids, 1.0, 0.0).astype(jnp.float32)
    return jnp.where(keeper[None], noise, 0.0) + identity[None] * diagonal_scale


def draw_lower_pivot(key, part):
    return triangle(jax.random.fold_in(key, 101), 2, KC, True).astype(jnp.bfloat16)


def draw_upper_pivot(key, part):
    return triangle(jax.random.fold_in(key, 103), 2, KC, False).astype(jnp.bfloat16)


def draw_parent_lower(key, part):
    return triangle(jax.random.fold_in(key, 107), 1, F, True).reshape(F, F).astype(jnp.bfloat16)


def draw_parent_upper(key, part):
    return triangle(jax.random.fold_in(key, 109), 1, F, False).reshape(F, F).astype(jnp.bfloat16)


def draw_maps(key, part):
    local = lax.broadcasted_iota(jnp.int32, (FU,), 0)
    first_bits = jax.random.randint(jax.random.fold_in(key, 211), (FU,), 0, 2)
    first_bits = jnp.where(local == 0, 0, first_bits)
    first_bits = jnp.where(local == FU - 1, 1, first_bits)
    second_bits = jax.random.randint(jax.random.fold_in(key, 212), (FU,), 0, 2)
    second_bits = jnp.where(local == 0, 1, second_bits)
    second_bits = jnp.where(local == FU - 1, 0, second_bits)
    return jnp.concatenate([2 * local + first_bits, 2 * local + second_bits]).astype(jnp.int32)


def levels(key, dims, shards, smallest, top_value):
    factor_of, own = 1.0, jax.random.fold_in(key, 6)
    for axis_at, blocks in shards:
        draws = jnp.exp(jax.random.uniform(jax.random.fold_in(own, axis_at), (blocks,), jnp.float32, smallest / len(shards), top_value / len(shards)))
        factor_of = factor_of * jnp.repeat(draws, dims[axis_at] // blocks).reshape([-1 if axis == axis_at else 1 for axis in range(len(dims))])
    return factor_of


def normal_values(stream_key, extent, spread, bound, pieces=(), held_as=jnp.bfloat16):
    level = levels(stream_key, extent, pieces, -0.22, 0.18) if pieces else 1.0
    drawn = jax.random.normal(stream_key, extent, jnp.float32) * spread * level
    return jnp.minimum(jnp.maximum(drawn, -bound), bound).astype(held_as)


def setup_inputs(seed: int = 0) -> dict:
    key_of = jax.random.split(jax.random.key(seed), 11)
    return {
        "pivot_rhs": normal_values(key_of[0], (2, KC, RHS), 1.0, 6.0, ((1, 8), (2, 4)), jnp.float32),
        "update_rhs": normal_values(key_of[1], (2 * FU, RHS), 1.0, 6.0, ((0, 8), (1, 4)), jnp.float32),
        "parent_rhs": normal_values(key_of[2], (F, RHS), 1.0, 6.0, ((0, 8), (1, 4)), jnp.float32),
        "lower_pivot": draw_lower_pivot(jax.random.fold_in(key_of[10], 71), 0),
        "lower_update": normal_values(key_of[4], (2 * FU, KC), KC ** -0.5, 0.125, ((0, 8), (1, 4))),
        "parent_lower": draw_parent_lower(jax.random.fold_in(key_of[10], 71), 0),
        "parent_upper": draw_parent_upper(jax.random.fold_in(key_of[10], 71), 0),
        "upper_pivot": draw_upper_pivot(jax.random.fold_in(key_of[10], 71), 0),
        "upper_update": normal_values(key_of[8], (2, KC, FU), FU ** -0.5, 0.125, ((1, 8), (2, 4))),
        "maps": draw_maps(jax.random.fold_in(key_of[10], 71), 0),
    }


def product(left, right):
    return jnp.dot(left, right, preferred_element_type=jnp.float32)


def reference(pivot_rhs, update_rhs, parent_rhs, lower_pivot, lower_update, parent_lower, parent_upper, upper_pivot, upper_update, maps):
    pivot_input = pivot_rhs.astype(jnp.bfloat16)
    solved = []
    updates = []
    for member in range(2):
        source = pivot_input[member]
        solved.append(product(lower_pivot[member], source))
        updates.append(update_rhs[member * FU:(member + 1) * FU] + product(lower_update[member * FU:(member + 1) * FU], source))
    pivot_half = jnp.stack(solved, axis=0).astype(jnp.bfloat16)
    update_half = jnp.concatenate(updates, axis=0).astype(jnp.bfloat16)
    widened = lax.optimization_barrier(update_half).astype(jnp.float32)
    scattered = jnp.zeros(parent_rhs.shape, jnp.float32).at[maps].add(widened)
    parent_sum = parent_rhs + scattered
    parent_mid = product(parent_lower, parent_sum.astype(jnp.bfloat16))
    parent_solution = product(parent_upper, parent_mid.astype(jnp.bfloat16))
    solution_half = parent_solution.astype(jnp.bfloat16)
    blocks = []
    for member in range(2):
        picked = jnp.take(solution_half, maps[member * FU:(member + 1) * FU], axis=0)
        direct = product(upper_pivot[member], pivot_half[member])
        blocks.append(direct + product(upper_update[member], picked))
    return parent_solution, jnp.stack(blocks, axis=0)
```

```python
import functools

import jax
import jax.numpy as jnp
from jax import lax
from jax.experimental import pallas as pl
from jax.experimental.pallas import tpu as pltpu
from jax.sharding import PartitionSpec as P

BF = jnp.bfloat16
F32 = jnp.float32
MESH = pl.DeviceIdType.MESH


def dot(left, right):
    return jnp.dot(left, right, preferred_element_type=F32)


def kernel(
    panels,
    cols,
    pivot_rhs,
    update_rhs,
    parent_rhs,
    lower_pivot,
    lower_update,
    parent_lower,
    parent_upper,
    upper_pivot,
    upper_update,
    row_map,
    col_map,
    parent_out,
    child_out,
    pin,
    phalf,
    vec,
    x_pin,
    x_half,
    x_par,
    s_up,
    r_up,
    s_piv,
    r_piv,
    s_par,
    r_par,
    s_ch,
    r_ch,
    uhalf,
    moved,
    picked,
    direct,
    g_send,
    g_recv,
    f_send,
    rs_send,
    rs_recv,
    sh_send,
    sh_recv,
):
    me_p, me_r = lax.axis_index("panel"), lax.axis_index("rhs")
    total = panels * cols
    me = me_p * cols + me_r
    core = lax.rem(me_p, 2)
    mate = me_p + 1 - 2 * core
    per = panels // cols
    half = panels // 2
    m = parent_rhs.shape[0]
    mk = pivot_rhs.shape[1]
    child = me_p // half

    barrier = pltpu.get_barrier_semaphore()

    @pl.loop(1, total)
    def _(step):
        other = lax.rem(me + step, total)
        pl.semaphore_signal(
            barrier,
            inc=1,
            device_id=(other // cols, lax.rem(other, cols)),
            device_id_type=MESH,
        )

    pin[...] = pivot_rhs[...].astype(BF)
    pl.semaphore_wait(barrier, total - 1)

    def spot(buffer, depth, column, part):
        return buffer.at[column, :, pl.ds(pl.multiple_of(part * depth, depth), depth), :]

    def send_copy(stage, block, buffer, depth, step):
        goal = lax.rem(me_p // 2 + step, half) * 2 + core
        return pltpu.make_async_remote_copy(
            src_ref=block,
            dst_ref=spot(buffer, depth, me_r, lax.rem(me_p, per)),
            send_sem=g_send.at[stage, step],
            recv_sem=g_recv.at[stage, me_r, lax.rem(me_p, per)],
            device_id=(goal, me_p // per),
            device_id_type=MESH,
        )

    def gather_start(stage, block, buffer, depth):
        for step in list(range(1, half)):
            send_copy(stage, block, buffer, depth, step).start()
        own = me_p // per == me_r

        @pl.when(own)
        def _():
            pltpu.make_async_copy(
                block,
                spot(buffer, depth, me_r, lax.rem(me_p, per)),
                g_recv.at[stage, me_r, lax.rem(me_p, per)],
            ).start()

        @pl.when(jnp.logical_not(own))
        def _():
            send_copy(stage, block, buffer, depth, 0).start()

    def gather_end(stage, block, buffer, depth):
        for step in range(1, half):
            send_copy(stage, block, buffer, depth, step).wait_send()

        @pl.when(me_p // per != me_r)
        def _():
            send_copy(stage, block, buffer, depth, 0).wait_send()

        for step in range(cols):
            for pair in range(per // 2):
                forward(stage, buffer, depth, step, pair).wait_send()

    def forward(stage, buffer, depth, step, pair):
        column = lax.rem(me_r + 1 + step, cols)
        part = 2 * pair + core
        place = spot(buffer, depth, column, part)
        return pltpu.make_async_remote_copy(
            src_ref=place,
            dst_ref=place,
            send_sem=f_send.at[stage, step, pair],
            recv_sem=g_recv.at[stage, column, part],
            device_id=(mate, me_r),
            device_id_type=MESH,
        )

    def landed(stage, buffer, depth, column, part):
        place = spot(buffer, depth, column, part)
        pltpu.make_async_copy(place, place, g_recv.at[stage, column, part]).wait()

    def pass_on(stage, buffer, depth):
        for step in range(cols):
            for pair in range(per // 2):
                column = lax.rem(me_r + 1 + step, cols)
                landed(stage, buffer, depth, column, 2 * pair + core)
                forward(stage, buffer, depth, step, pair).start()

    def arrive(stage, buffer, depth, step):
        column = lax.rem(me_r + 1 + step, cols)
        for pair in range(per // 2):
            landed(stage, buffer, depth, column, 2 * pair + 1 - core)
        return column

    def scatter_copy(stage, source, target, step):
        return pltpu.make_async_remote_copy(
            src_ref=source.at[step],
            dst_ref=target.at[step],
            send_sem=rs_send.at[stage, step],
            recv_sem=rs_recv.at[stage, step],
            device_id=(me_p, lax.rem(me_r + 1 + step, cols)),
            device_id_type=MESH,
        )

    def scatter_sum(stage, source, target, value):
        for step in range(cols - 1):
            scatter_copy(stage, source, target, step).wait_recv()
            value = value + target[step].astype(F32)
        for step in range(cols - 1):
            scatter_copy(stage, source, target, step).wait_send()
        return value

    last = cols - 1

    gather_start(0, pin, x_pin, mk)

    width = upper_update.shape[2]
    for k in range(2):
        rows = lax.broadcasted_iota(jnp.int32, (per * m, width), 0)
        chosen = (rows == col_map[k : k + 1, :]).astype(F32).astype(BF)
        picked[k] = lax.dot_general(
            upper_update[k], chosen, (((1,), (1,)), ((), ())), preferred_element_type=F32
        ).astype(BF)

    pass_on(0, x_pin, mk)
    update = update_rhs[...]
    for step in range(cols):
        column = arrive(0, x_pin, mk, step)
        value = dot(lower_update[...], x_pin[column, child])
        if step < last:
            s_up[step] = value.astype(BF)
            scatter_copy(0, s_up, r_up, step).start()
        else:
            update = update + value
    for step in range(cols):
        column = lax.rem(me_r + 1 + step, cols)
        for k in range(2):
            value = dot(lower_pivot[k], x_pin[column, k])
            if step < last:
                s_piv[step, k] = value.astype(BF)
            else:
                direct[step, k] = value
        if step < last:
            scatter_copy(1, s_piv, r_piv, step).start()
    gather_end(0, pin, x_pin, mk)
    update = scatter_sum(0, s_up, r_up, update).astype(BF)
    uhalf[0] = update[: m // 2]
    uhalf[1] = update[m // 2 :]
    first = lax.rem(me_p, half) * 2

    def shuffle(side):
        return pltpu.make_async_remote_copy(
            src_ref=uhalf.at[side],
            dst_ref=moved.at[child],
            send_sem=sh_send.at[side],
            recv_sem=sh_recv.at[child],
            device_id=(first + side, me_r),
            device_id_type=MESH,
        )

    for side in range(2):

        @pl.when(first + side != me_p)
        def _():
            shuffle(side).start()

        @pl.when(first + side == me_p)
        def _():
            pltpu.make_async_copy(uhalf.at[side], moved.at[child], sh_recv.at[child]).start()

    phalf[...] = scatter_sum(1, s_piv, r_piv, direct[last]).astype(BF)
    rows = lax.broadcasted_iota(jnp.int32, (m, m // 2), 0)
    spread = parent_rhs[...]
    for k in range(2):
        pltpu.make_async_copy(moved.at[k], moved.at[k], sh_recv.at[k]).wait()
        chosen = (rows == row_map[k : k + 1, :]).astype(F32).astype(BF)
        spread = spread + dot(chosen, moved[k])
    vec[0, 0] = spread.astype(BF)
    for side in range(2):

        @pl.when(first + side != me_p)
        def _():
            shuffle(side).wait_send()

    gather_start(1, vec.at[0], x_par.at[0], m)
    gather_start(2, phalf, x_half, mk)

    for level, factor in ((0, parent_lower), (1, parent_upper)):
        stage = 1 if level == 0 else 3
        block, buffer = vec.at[level], x_par.at[level]
        pass_on(stage, buffer, m)
        value = None
        for step in range(cols):
            column = arrive(stage, buffer, m, step)
            value = dot(factor[...], x_par[level, column, 0])
            if step < last:
                s_par[level, step] = value.astype(BF)
                scatter_copy(2 + level, s_par.at[level], r_par.at[level], step).start()
        gather_end(stage, block, buffer, m)
        value = scatter_sum(2 + level, s_par.at[level], r_par.at[level], value)
        vec[level + 1, 0] = value.astype(BF)
        following = 3 if level == 0 else 4
        gather_start(following, vec.at[level + 1], x_par.at[level + 1], m)
        if level == 0:
            pass_on(2, x_half, mk)
            for step in range(cols):
                column = arrive(2, x_half, mk, step)
                for k in range(2):
                    direct[step, k] = dot(upper_pivot[k], x_half[column, k])
            gather_end(2, phalf, x_half, mk)
        else:
            parent_out[...] = value

    pass_on(4, x_par.at[2], m)
    for step in range(cols):
        column = arrive(4, x_par.at[2], m, step)
        for k in range(2):
            value = direct[step, k] + dot(picked[k], x_par[2, column, 0])
            if step < last:
                s_ch[step, k] = value.astype(BF)
            else:
                direct[step, k] = value
        if step < last:
            scatter_copy(4, s_ch, r_ch, step).start()
    gather_end(4, vec.at[2], x_par.at[2], m)
    child_out[...] = scatter_sum(4, s_ch, r_ch, direct[last])


def shards(panels, cols, *arguments):
    *arrays, maps = arguments
    m, width = arrays[1].shape
    mk = arrays[0].shape[1]
    per = panels // cols
    sides = maps.reshape(2, -1)
    me_p, me_r = lax.axis_index("panel"), lax.axis_index("rhs")
    row_map = lax.dynamic_slice_in_dim(sides, me_p * (m // 2), m // 2, 1) - me_p * m
    wide = arrays[8].shape[2]
    col_map = lax.dynamic_slice_in_dim(sides, me_r * wide, wide, 1) - me_r * per * m
    vm = pltpu.VMEM
    dma = pltpu.SemaphoreType.DMA
    return pl.pallas_call(
        functools.partial(kernel, panels, cols),
        out_shape=(
            jax.ShapeDtypeStruct((m, width), F32),
            jax.ShapeDtypeStruct((2, mk, width), F32),
        ),
        in_specs=[pl.BlockSpec(memory_space=pltpu.VMEM)] * 11,
        out_specs=(pl.BlockSpec(memory_space=pltpu.VMEM),) * 2,
        scratch_shapes=[
            vm((2, mk, width), BF),
            vm((2, mk, width), BF),
            vm((3, 1, m, width), BF),
            vm((cols, 2, per * mk, width), BF),
            vm((cols, 2, per * mk, width), BF),
            vm((3, cols, 1, per * m, width), BF),
            vm((cols - 1, m, width), BF),
            vm((cols - 1, m, width), BF),
            vm((cols - 1, 2, mk, width), BF),
            vm((cols - 1, 2, mk, width), BF),
            vm((2, cols - 1, m, width), BF),
            vm((2, cols - 1, m, width), BF),
            vm((cols - 1, 2, mk, width), BF),
            vm((cols - 1, 2, mk, width), BF),
            vm((2, m // 2, width), BF),
            vm((2, m // 2, width), BF),
            vm((2, mk, per * m), BF),
            vm((cols, 2, mk, width), F32),
            dma((5, panels // 2)),
            dma((5, cols, per)),
            dma((5, cols, per // 2)),
            dma((5, cols - 1)),
            dma((5, cols - 1)),
            dma((2,)),
            dma((2,)),
        ],
        compiler_params=pltpu.CompilerParams(
            collective_id=0, has_side_effects=True, vmem_limit_bytes=60 * 1024 * 1024
        ),
    )(*arrays, row_map, col_map)


def solution(mesh):
    panels, cols = mesh.shape["panel"], mesh.shape["rhs"]
    placed = (
        P(None, "panel", "rhs"),
        P("panel", "rhs"),
        P("panel", "rhs"),
        P(None, "panel", "rhs"),
        P("panel", "rhs"),
        P("panel", "rhs"),
        P("panel", "rhs"),
        P(None, "panel", "rhs"),
        P(None, "panel", "rhs"),
        P(),
    )
    return jax.shard_map(
        functools.partial(shards, panels, cols),
        mesh=mesh,
        in_specs=placed,
        out_specs=(P("panel", "rhs"), P(None, "panel", "rhs")),
        check_vma=False,
    )
```

```python
import functools

import jax
import jax.numpy as jnp
from jax import lax
from jax.experimental import pallas as pl
from jax.experimental.pallas import tpu as pltpu
from jax.sharding import PartitionSpec as P

BF = jnp.bfloat16
F32 = jnp.float32
MESH = pl.DeviceIdType.MESH


def dot(left, right):
    return jnp.dot(left, right, preferred_element_type=F32)


def kernel(
    panels,
    cols,
    pivot_rhs,
    update_rhs,
    parent_rhs,
    lower_pivot,
    lower_update,
    parent_lower,
    parent_upper,
    upper_pivot,
    upper_update,
    row_map,
    col_map,
    parent_out,
    child_out,
    pin,
    phalf,
    vec,
    x_pin,
    x_half,
    x_par,
    s_up,
    r_up,
    s_piv,
    r_piv,
    s_par,
    r_par,
    s_ch,
    r_ch,
    uhalf,
    moved,
    picked,
    direct,
    par_sum,
    spread_sum,
    child_sum,
    g_send,
    g_recv,
    f_send,
    rs_send,
    rs_recv,
    sh_send,
    sh_recv,
):
    me_p, me_r = lax.axis_index("panel"), lax.axis_index("rhs")
    total = panels * cols
    me = me_p * cols + me_r
    core = lax.rem(me_p, 2)
    mate = me_p + 1 - 2 * core
    per = panels // cols
    half = panels // 2
    m = parent_rhs.shape[0]
    mk = pivot_rhs.shape[1]
    child = me_p // half

    barrier = pltpu.get_barrier_semaphore()

    @pl.loop(1, total)
    def _(step):
        other = lax.rem(me + step, total)
        pl.semaphore_signal(
            barrier,
            inc=1,
            device_id=(other // cols, lax.rem(other, cols)),
            device_id_type=MESH,
        )

    pin[...] = pivot_rhs[...].astype(BF)
    direct[...] = jnp.zeros_like(direct)
    pl.semaphore_wait(barrier, total - 1)

    group = me_p // per
    last = cols - 1

    def every(source, goal):
        return None

    def below(source, goal):
        return goal >= source

    def above(source, goal):
        return goal <= source

    def guard(condition, action):
        if condition is None:
            action()
        else:
            pl.when(condition)(action)

    def both(first, second):
        return second if first is None else jnp.logical_and(first, second)

    def spot(buffer, depth, column, part, lead):
        rows = pl.ds(pl.multiple_of(part * depth, depth), depth)
        return buffer.at[column, slice(None) if lead is None else pl.ds(lead, 1), rows, :]

    class Gather:
        def __init__(self, stage, block, buffer, depth, keep, lead):
            self.stage, self.block, self.buffer, self.depth = stage, block, buffer, depth
            self.keep, self.lead = keep, lead
            self.active = keep(me_r, group)

        def place(self, column, part, panel):
            return spot(self.buffer, self.depth, column, part, self.lead(panel))

        def piece(self, panel):
            lead = self.lead(panel)
            return self.block if lead is None else self.block.at[pl.ds(lead, 1)]

        def goal(self, step):
            return lax.rem(me_p // 2 + step, half) * 2 + core

        def copy(self, step):
            goal = self.goal(step)
            return pltpu.make_async_remote_copy(
                src_ref=self.piece(goal),
                dst_ref=self.place(me_r, lax.rem(me_p, per), goal),
                send_sem=g_send.at[self.stage, step],
                recv_sem=g_recv.at[self.stage, me_r, lax.rem(me_p, per)],
                device_id=(goal, group),
                device_id_type=MESH,
            )

        def sends(self, action):
            for step in list(range(1, half)) + [0]:
                condition = self.keep(group, self.goal(step) // per)
                if step == 0:
                    condition = both(condition, group != me_r)
                guard(condition, functools.partial(action, step))

        def start(self):
            self.sends(lambda step: self.copy(step).start())

            @pl.when(group == me_r)
            def _():
                part = lax.rem(me_p, per)
                pltpu.make_async_copy(
                    self.piece(me_p),
                    self.place(me_r, part, me_p),
                    g_recv.at[self.stage, me_r, part],
                ).start()

        def landed(self, column, part):
            place = self.place(column, part, me_p)
            pltpu.make_async_copy(place, place, g_recv.at[self.stage, column, part]).wait()

        def forward(self, step, pair):
            column = lax.rem(me_r + 1 + step, cols)
            part = 2 * pair + core
            return pltpu.make_async_remote_copy(
                src_ref=self.place(column, part, me_p),
                dst_ref=self.place(column, part, me_p),
                send_sem=f_send.at[self.stage, step, pair],
                recv_sem=g_recv.at[self.stage, column, part],
                device_id=(mate, me_r),
                device_id_type=MESH,
            )

        def pass_on(self):
            def action():
                for step in range(cols):
                    for pair in range(per // 2):
                        self.landed(lax.rem(me_r + 1 + step, cols), 2 * pair + core)
                        self.forward(step, pair).start()

            guard(self.active, action)

        def arrive(self, step):
            column = lax.rem(me_r + 1 + step, cols)
            for pair in range(per // 2):
                self.landed(column, 2 * pair + 1 - core)
            return column

        def finish(self):
            self.sends(lambda step: self.copy(step).wait_send())

            def action():
                for step in range(cols):
                    for pair in range(per // 2):
                        self.forward(step, pair).wait_send()

            guard(self.active, action)

    class Scatter:
        def __init__(self, stage, source, target, keep):
            self.stage, self.source, self.target, self.keep = stage, source, target, keep
            self.active = keep(me_r, group)

        def copy(self, step):
            return pltpu.make_async_remote_copy(
                src_ref=self.source.at[step],
                dst_ref=self.target.at[step],
                send_sem=rs_send.at[self.stage, step],
                recv_sem=rs_recv.at[self.stage, step],
                device_id=(me_p, lax.rem(me_r + 1 + step, cols)),
                device_id_type=MESH,
            )

        def add(self, total_ref):
            for step in range(last):
                sender = lax.rem(me_r + last - step, cols)

                def action(step=step):
                    self.copy(step).wait_recv()
                    total_ref[...] += self.target[step].astype(F32)

                guard(self.keep(sender, group), action)

        def finish(self):
            def action():
                for step in range(last):
                    self.copy(step).wait_send()

            guard(self.active, action)

    def whole(panel):
        return None

    def same(panel):
        return panel // half

    def other(panel):
        return 1 - panel // half

    g_own = Gather(0, pin, x_pin, mk, every, same)
    g_other = Gather(5, pin, x_pin, mk, below, other)
    g_low = Gather(1, vec.at[0], x_par.at[0], m, below, whole)
    g_half = Gather(2, phalf, x_half, mk, above, whole)
    g_up = Gather(3, vec.at[1], x_par.at[1], m, above, whole)
    g_all = Gather(4, vec.at[2], x_par.at[2], m, every, whole)
    t_up = Scatter(0, s_up, r_up, every)
    t_piv = Scatter(1, s_piv, r_piv, below)
    t_low = Scatter(2, s_par.at[0], r_par.at[0], below)
    t_high = Scatter(3, s_par.at[1], r_par.at[1], above)
    t_child = Scatter(4, s_ch, r_ch, every)

    g_own.start()
    g_other.start()

    width = upper_update.shape[2]
    for k in range(2):
        rows = lax.broadcasted_iota(jnp.int32, (per * m, width), 0)
        chosen = (rows == col_map[k : k + 1, :]).astype(F32).astype(BF)
        picked[k] = lax.dot_general(
            upper_update[k], chosen, (((1,), (1,)), ((), ())), preferred_element_type=F32
        ).astype(BF)
    spread_sum[...] = parent_rhs[...]

    g_own.pass_on()
    for step in range(cols):
        column = g_own.arrive(step)
        value = dot(lower_update[...], x_pin[column, child])
        if step < last:
            s_up[step] = value.astype(BF)
            t_up.copy(step).start()
        else:
            par_sum[...] = update_rhs[...] + value
    g_other.pass_on()
    t_up.add(par_sum)
    update = par_sum[...].astype(BF)
    uhalf[0] = update[: m // 2]
    uhalf[1] = update[m // 2 :]
    first = lax.rem(me_p, half) * 2

    def shuffle(side):
        return pltpu.make_async_remote_copy(
            src_ref=uhalf.at[side],
            dst_ref=moved.at[child],
            send_sem=sh_send.at[side],
            recv_sem=sh_recv.at[child],
            device_id=(first + side, me_r),
            device_id_type=MESH,
        )

    for side in range(2):

        @pl.when(first + side != me_p)
        def _():
            shuffle(side).start()

        @pl.when(first + side == me_p)
        def _():
            pltpu.make_async_copy(uhalf.at[side], moved.at[child], sh_recv.at[child]).start()

    child_sum[...] = jnp.zeros_like(child_sum)

    def pivots():
        for step in range(cols):
            column = g_other.arrive(step)
            for k in range(2):
                value = dot(lower_pivot[k], x_pin[column, k])
                if step < last:
                    s_piv[step, k] = value.astype(BF)
                else:
                    child_sum[k] = value
            if step < last:
                t_piv.copy(step).start()

    guard(g_other.active, pivots)

    rows = lax.broadcasted_iota(jnp.int32, (m, m // 2), 0)
    for k in range(2):
        pltpu.make_async_copy(moved.at[k], moved.at[k], sh_recv.at[k]).wait()
        chosen = (rows == row_map[k : k + 1, :]).astype(F32).astype(BF)
        spread_sum[...] += dot(chosen, moved[k])
    vec[0, 0] = spread_sum[...].astype(BF)
    g_low.start()

    t_piv.add(child_sum)
    phalf[...] = child_sum[...].astype(BF)
    g_half.start()

    def parent(level, gather, scatter, factor):
        par_sum[...] = jnp.zeros_like(par_sum)
        gather.pass_on()

        def action():
            for step in range(cols):
                column = gather.arrive(step)
                value = dot(factor[...], x_par[level, column, 0])
                if step < last:
                    s_par[level, step] = value.astype(BF)
                    scatter.copy(step).start()
                else:
                    par_sum[...] = value

        guard(gather.active, action)
        scatter.add(par_sum)
        vec[level + 1, 0] = par_sum[...].astype(BF)

    parent(0, g_low, t_low, parent_lower)
    g_up.start()
    g_half.pass_on()

    def known():
        for step in range(cols):
            column = g_half.arrive(step)
            for k in range(2):
                direct[step, k] = dot(upper_pivot[k], x_half[column, k])

    guard(g_half.active, known)
    parent(1, g_up, t_high, parent_upper)
    g_all.start()
    parent_out[...] = par_sum[...]

    g_all.pass_on()
    for step in range(cols):
        column = g_all.arrive(step)
        for k in range(2):
            value = direct[step, k] + dot(picked[k], x_par[2, column, 0])
            if step < last:
                s_ch[step, k] = value.astype(BF)
            else:
                child_out[k] = value
        if step < last:
            t_child.copy(step).start()
    for gather in (g_own, g_other, g_low, g_half, g_up, g_all):
        gather.finish()
    for side in range(2):

        @pl.when(first + side != me_p)
        def _():
            shuffle(side).wait_send()

    t_child.add(child_out)
    for scatter in (t_up, t_piv, t_low, t_high, t_child):
        scatter.finish()


def shards(panels, cols, *arguments):
    *arrays, maps = arguments
    m, width = arrays[1].shape
    mk = arrays[0].shape[1]
    per = panels // cols
    sides = maps.reshape(2, -1)
    me_p, me_r = lax.axis_index("panel"), lax.axis_index("rhs")
    row_map = lax.dynamic_slice_in_dim(sides, me_p * (m // 2), m // 2, 1) - me_p * m
    wide = arrays[8].shape[2]
    col_map = lax.dynamic_slice_in_dim(sides, me_r * wide, wide, 1) - me_r * per * m
    vm = pltpu.VMEM
    dma = pltpu.SemaphoreType.DMA
    return pl.pallas_call(
        functools.partial(kernel, panels, cols),
        out_shape=(
            jax.ShapeDtypeStruct((m, width), F32),
            jax.ShapeDtypeStruct((2, mk, width), F32),
        ),
        in_specs=[pl.BlockSpec(memory_space=pltpu.VMEM)] * 11,
        out_specs=(pl.BlockSpec(memory_space=pltpu.VMEM),) * 2,
        scratch_shapes=[
            vm((2, mk, width), BF),
            vm((2, mk, width), BF),
            vm((3, 1, m, width), BF),
            vm((cols, 2, per * mk, width), BF),
            vm((cols, 2, per * mk, width), BF),
            vm((3, cols, 1, per * m, width), BF),
            vm((cols - 1, m, width), BF),
            vm((cols - 1, m, width), BF),
            vm((cols - 1, 2, mk, width), BF),
            vm((cols - 1, 2, mk, width), BF),
            vm((2, cols - 1, m, width), BF),
            vm((2, cols - 1, m, width), BF),
            vm((cols - 1, 2, mk, width), BF),
            vm((cols - 1, 2, mk, width), BF),
            vm((2, m // 2, width), BF),
            vm((2, m // 2, width), BF),
            vm((2, mk, per * m), BF),
            vm((cols, 2, mk, width), F32),
            vm((m, width), F32),
            vm((m, width), F32),
            vm((2, mk, width), F32),
            dma((6, panels // 2)),
            dma((6, cols, per)),
            dma((6, cols, per // 2)),
            dma((5, cols - 1)),
            dma((5, cols - 1)),
            dma((2,)),
            dma((2,)),
        ],
        compiler_params=pltpu.CompilerParams(
            collective_id=0, has_side_effects=True, vmem_limit_bytes=60 * 1024 * 1024
        ),
    )(*arrays, row_map, col_map)


def solution(mesh):
    panels, cols = mesh.shape["panel"], mesh.shape["rhs"]
    placed = (
        P(None, "panel", "rhs"),
        P("panel", "rhs"),
        P("panel", "rhs"),
        P(None, "panel", "rhs"),
        P("panel", "rhs"),
        P("panel", "rhs"),
        P("panel", "rhs"),
        P(None, "panel", "rhs"),
        P(None, "panel", "rhs"),
        P(),
    )
    return jax.shard_map(
        functools.partial(shards, panels, cols),
        mesh=mesh,
        in_specs=placed,
        out_specs=(P("panel", "rhs"), P(None, "panel", "rhs")),
        check_vma=False,
    )
```

```python
import functools

import jax
import jax.numpy as jnp
from jax import lax
from jax.experimental import pallas as pl
from jax.experimental.pallas import tpu as pltpu
from jax.sharding import PartitionSpec as P

BF = jnp.bfloat16
F32 = jnp.float32
MESH = pl.DeviceIdType.MESH


def dot(left, right):
    return jnp.dot(left, right, preferred_element_type=F32)


def kernel(
    panels,
    cols,
    pivot_rhs,
    update_rhs,
    parent_rhs,
    lower_pivot,
    lower_update,
    parent_lower,
    parent_upper,
    upper_pivot,
    upper_update,
    row_map,
    col_map,
    parent_out,
    child_out,
    pin,
    phalf,
    vec,
    x_pin,
    x_half,
    x_par,
    s_up,
    r_up,
    s_piv,
    r_piv,
    s_par,
    r_par,
    s_ch,
    r_ch,
    uhalf,
    moved,
    picked,
    direct,
    par_sum,
    spread_sum,
    child_sum,
    g_send,
    g_recv,
    f_send,
    rs_send,
    rs_recv,
    sh_send,
    sh_recv,
):
    me_p, me_r = lax.axis_index("panel"), lax.axis_index("rhs")
    total = panels * cols
    me = me_p * cols + me_r
    core = lax.rem(me_p, 2)
    mate = me_p + 1 - 2 * core
    per = panels // cols
    half = panels // 2
    m = parent_rhs.shape[0]
    mk = pivot_rhs.shape[1]
    child = me_p // half

    barrier = pltpu.get_barrier_semaphore()

    @pl.loop(1, total)
    def _(step):
        other = lax.rem(me + step, total)
        pl.semaphore_signal(
            barrier,
            inc=1,
            device_id=(other // cols, lax.rem(other, cols)),
            device_id_type=MESH,
        )

    pin[...] = pivot_rhs[...].astype(BF)
    direct[...] = jnp.zeros_like(direct)
    pl.semaphore_wait(barrier, total - 1)

    group = me_p // per
    last = cols - 1

    def every(source, goal):
        return None

    def below(source, goal):
        return goal >= source

    def above(source, goal):
        return goal <= source

    def guard(condition, action):
        if condition is None:
            action()
        else:
            pl.when(condition)(action)

    def both(first, second):
        return second if first is None else jnp.logical_and(first, second)

    def spot(buffer, depth, column, part, lead):
        rows = pl.ds(pl.multiple_of(part * depth, depth), depth)
        return buffer.at[column, slice(None) if lead is None else pl.ds(lead, 1), rows, :]

    class Gather:
        def __init__(self, stage, block, buffer, depth, keep, lead):
            self.stage, self.block, self.buffer, self.depth = stage, block, buffer, depth // 2
            self.keep, self.lead = keep, lead
            self.active = keep(me_r, group)

        def place(self, column, part, panel):
            return spot(self.buffer, self.depth, column, part, self.lead(panel))

        def piece(self, panel, sub):
            lead = self.lead(panel)
            rows = pl.ds(sub * self.depth, self.depth)
            return self.block.at[slice(None) if lead is None else pl.ds(lead, 1), rows, :]

        def goal(self, step):
            return lax.rem(me_p // 2 + step, half) * 2 + core

        def copy(self, step, sub):
            goal = self.goal(step)
            part = 2 * lax.rem(me_p, per) + sub
            return pltpu.make_async_remote_copy(
                src_ref=self.piece(goal, sub),
                dst_ref=self.place(me_r, part, goal),
                send_sem=g_send.at[self.stage, step, sub],
                recv_sem=g_recv.at[self.stage, me_r, part],
                device_id=(goal, group),
                device_id_type=MESH,
            )

        def sends(self, action):
            for step in list(range(1, half)) + [0]:
                condition = self.keep(group, self.goal(step) // per)
                if step == 0:
                    condition = both(condition, group != me_r)
                guard(condition, functools.partial(action, step))

        def start(self):
            def action(step):
                for sub in range(2):
                    self.copy(step, sub).start()

            self.sends(action)

            @pl.when(group == me_r)
            def _():
                for sub in range(2):
                    part = 2 * lax.rem(me_p, per) + sub
                    pltpu.make_async_copy(
                        self.piece(me_p, sub),
                        self.place(me_r, part, me_p),
                        g_recv.at[self.stage, me_r, part],
                    ).start()

        def landed(self, column, part):
            place = self.place(column, part, me_p)
            pltpu.make_async_copy(place, place, g_recv.at[self.stage, column, part]).wait()

        def forward(self, step, pair, sub):
            column = lax.rem(me_r + 1 + step, cols)
            part = 4 * pair + 2 * core + sub
            return pltpu.make_async_remote_copy(
                src_ref=self.place(column, part, me_p),
                dst_ref=self.place(column, part, me_p),
                send_sem=f_send.at[self.stage, step, 2 * pair + sub],
                recv_sem=g_recv.at[self.stage, column, part],
                device_id=(mate, me_r),
                device_id_type=MESH,
            )

        def pass_on(self):
            def action():
                for sub in range(2):
                    for step in range(cols):
                        for pair in range(per // 2):
                            column = lax.rem(me_r + 1 + step, cols)
                            self.landed(column, 4 * pair + 2 * core + sub)
                            self.forward(step, pair, sub).start()

            guard(self.active, action)

        def arrive(self, step):
            column = lax.rem(me_r + 1 + step, cols)
            for pair in range(per // 2):
                for sub in range(2):
                    self.landed(column, 4 * pair + 2 * (1 - core) + sub)
            return column

        def finish(self):
            def sent(step):
                for sub in range(2):
                    self.copy(step, sub).wait_send()

            self.sends(sent)

            def action():
                for step in range(cols):
                    for pair in range(per // 2):
                        for sub in range(2):
                            self.forward(step, pair, sub).wait_send()

            guard(self.active, action)

    class Scatter:
        def __init__(self, stage, source, target, keep):
            self.stage, self.source, self.target, self.keep = stage, source, target, keep
            self.active = keep(me_r, group)

        def copy(self, step):
            return pltpu.make_async_remote_copy(
                src_ref=self.source.at[step],
                dst_ref=self.target.at[step],
                send_sem=rs_send.at[self.stage, step],
                recv_sem=rs_recv.at[self.stage, step],
                device_id=(me_p, lax.rem(me_r + 1 + step, cols)),
                device_id_type=MESH,
            )

        def add(self, total_ref):
            for step in range(last):
                sender = lax.rem(me_r + last - step, cols)

                def action(step=step):
                    self.copy(step).wait_recv()
                    total_ref[...] += self.target[step].astype(F32)

                guard(self.keep(sender, group), action)

        def finish(self):
            def action():
                for step in range(last):
                    self.copy(step).wait_send()

            guard(self.active, action)

    def whole(panel):
        return None

    def same(panel):
        return panel // half

    def other(panel):
        return 1 - panel // half

    g_own = Gather(0, pin, x_pin, mk, every, same)
    g_other = Gather(5, pin, x_pin, mk, below, other)
    g_low = Gather(1, vec.at[0], x_par.at[0], m, below, whole)
    g_half = Gather(2, phalf, x_half, mk, above, whole)
    g_up = Gather(3, vec.at[1], x_par.at[1], m, above, whole)
    g_all = Gather(4, vec.at[2], x_par.at[2], m, every, whole)
    t_up = Scatter(0, s_up, r_up, every)
    t_piv = Scatter(1, s_piv, r_piv, below)
    t_low = Scatter(2, s_par.at[0], r_par.at[0], below)
    t_high = Scatter(3, s_par.at[1], r_par.at[1], above)
    t_child = Scatter(4, s_ch, r_ch, every)

    g_own.start()
    g_other.start()

    width = upper_update.shape[2]
    for k in range(2):
        rows = lax.broadcasted_iota(jnp.int32, (per * m, width), 0)
        chosen = (rows == col_map[k : k + 1, :]).astype(F32).astype(BF)
        picked[k] = lax.dot_general(
            upper_update[k], chosen, (((1,), (1,)), ((), ())), preferred_element_type=F32
        ).astype(BF)
    spread_sum[...] = parent_rhs[...]

    g_own.pass_on()
    for step in range(cols):
        column = g_own.arrive(step)
        value = dot(lower_update[...], x_pin[column, child])
        if step < last:
            s_up[step] = value.astype(BF)
            t_up.copy(step).start()
        else:
            par_sum[...] = update_rhs[...] + value
    g_other.pass_on()
    t_up.add(par_sum)
    update = par_sum[...].astype(BF)
    uhalf[0] = update[: m // 2]
    uhalf[1] = update[m // 2 :]
    first = lax.rem(me_p, half) * 2

    def shuffle(side):
        return pltpu.make_async_remote_copy(
            src_ref=uhalf.at[side],
            dst_ref=moved.at[child],
            send_sem=sh_send.at[side],
            recv_sem=sh_recv.at[child],
            device_id=(first + side, me_r),
            device_id_type=MESH,
        )

    for side in range(2):

        @pl.when(first + side != me_p)
        def _():
            shuffle(side).start()

        @pl.when(first + side == me_p)
        def _():
            pltpu.make_async_copy(uhalf.at[side], moved.at[child], sh_recv.at[child]).start()

    child_sum[...] = jnp.zeros_like(child_sum)

    def pivots():
        for step in range(cols):
            column = g_other.arrive(step)
            for k in range(2):
                value = dot(lower_pivot[k], x_pin[column, k])
                if step < last:
                    s_piv[step, k] = value.astype(BF)
                else:
                    child_sum[k] = value
            if step < last:
                t_piv.copy(step).start()

    guard(g_other.active, pivots)

    rows = lax.broadcasted_iota(jnp.int32, (m, m // 2), 0)
    for k in range(2):
        pltpu.make_async_copy(moved.at[k], moved.at[k], sh_recv.at[k]).wait()
        chosen = (rows == row_map[k : k + 1, :]).astype(F32).astype(BF)
        spread_sum[...] += dot(chosen, moved[k])
    vec[0, 0] = spread_sum[...].astype(BF)
    g_low.start()

    t_piv.add(child_sum)
    phalf[...] = child_sum[...].astype(BF)
    g_half.start()

    def parent(level, gather, scatter, factor):
        par_sum[...] = jnp.zeros_like(par_sum)
        gather.pass_on()

        def action():
            for step in range(cols):
                column = gather.arrive(step)
                value = dot(factor[...], x_par[level, column, 0])
                if step < last:
                    s_par[level, step] = value.astype(BF)
                    scatter.copy(step).start()
                else:
                    par_sum[...] = value

        guard(gather.active, action)
        scatter.add(par_sum)
        vec[level + 1, 0] = par_sum[...].astype(BF)

    parent(0, g_low, t_low, parent_lower)
    g_up.start()
    g_half.pass_on()

    def known():
        for step in range(cols):
            column = g_half.arrive(step)
            for k in range(2):
                direct[step, k] = dot(upper_pivot[k], x_half[column, k])

    guard(g_half.active, known)
    parent(1, g_up, t_high, parent_upper)
    g_all.start()
    parent_out[...] = par_sum[...]

    g_all.pass_on()
    for step in range(cols):
        column = g_all.arrive(step)
        for k in range(2):
            value = direct[step, k] + dot(picked[k], x_par[2, column, 0])
            if step < last:
                s_ch[step, k] = value.astype(BF)
            else:
                child_out[k] = value
        if step < last:
            t_child.copy(step).start()
    for gather in (g_own, g_other, g_low, g_half, g_up, g_all):
        gather.finish()
    for side in range(2):

        @pl.when(first + side != me_p)
        def _():
            shuffle(side).wait_send()

    t_child.add(child_out)
    for scatter in (t_up, t_piv, t_low, t_high, t_child):
        scatter.finish()


def shards(panels, cols, *arguments):
    *arrays, maps = arguments
    m, width = arrays[1].shape
    mk = arrays[0].shape[1]
    per = panels // cols
    sides = maps.reshape(2, -1)
    me_p, me_r = lax.axis_index("panel"), lax.axis_index("rhs")
    row_map = lax.dynamic_slice_in_dim(sides, me_p * (m // 2), m // 2, 1) - me_p * m
    wide = arrays[8].shape[2]
    col_map = lax.dynamic_slice_in_dim(sides, me_r * wide, wide, 1) - me_r * per * m
    vm = pltpu.VMEM
    dma = pltpu.SemaphoreType.DMA
    return pl.pallas_call(
        functools.partial(kernel, panels, cols),
        out_shape=(
            jax.ShapeDtypeStruct((m, width), F32),
            jax.ShapeDtypeStruct((2, mk, width), F32),
        ),
        in_specs=[pl.BlockSpec(memory_space=pltpu.VMEM)] * 11,
        out_specs=(pl.BlockSpec(memory_space=pltpu.VMEM),) * 2,
        scratch_shapes=[
            vm((2, mk, width), BF),
            vm((2, mk, width), BF),
            vm((3, 1, m, width), BF),
            vm((cols, 2, per * mk, width), BF),
            vm((cols, 2, per * mk, width), BF),
            vm((3, cols, 1, per * m, width), BF),
            vm((cols - 1, m, width), BF),
            vm((cols - 1, m, width), BF),
            vm((cols - 1, 2, mk, width), BF),
            vm((cols - 1, 2, mk, width), BF),
            vm((2, cols - 1, m, width), BF),
            vm((2, cols - 1, m, width), BF),
            vm((cols - 1, 2, mk, width), BF),
            vm((cols - 1, 2, mk, width), BF),
            vm((2, m // 2, width), BF),
            vm((2, m // 2, width), BF),
            vm((2, mk, per * m), BF),
            vm((cols, 2, mk, width), F32),
            vm((m, width), F32),
            vm((m, width), F32),
            vm((2, mk, width), F32),
            dma((6, panels // 2, 2)),
            dma((6, cols, 2 * per)),
            dma((6, cols, per)),
            dma((5, cols - 1)),
            dma((5, cols - 1)),
            dma((2,)),
            dma((2,)),
        ],
        compiler_params=pltpu.CompilerParams(
            collective_id=0, has_side_effects=True, vmem_limit_bytes=60 * 1024 * 1024
        ),
    )(*arrays, row_map, col_map)


def solution(mesh):
    panels, cols = mesh.shape["panel"], mesh.shape["rhs"]
    placed = (
        P(None, "panel", "rhs"),
        P("panel", "rhs"),
        P("panel", "rhs"),
        P(None, "panel", "rhs"),
        P("panel", "rhs"),
        P("panel", "rhs"),
        P("panel", "rhs"),
        P(None, "panel", "rhs"),
        P(None, "panel", "rhs"),
        P(),
    )
    return jax.shard_map(
        functools.partial(shards, panels, cols),
        mesh=mesh,
        in_specs=placed,
        out_specs=(P("panel", "rhs"), P(None, "panel", "rhs")),
        check_vma=False,
    )
```

```python
import functools

import jax
import jax.numpy as jnp
from jax import lax
from jax.experimental import pallas as pl
from jax.experimental.pallas import tpu as pltpu
from jax.sharding import PartitionSpec as P

BF = jnp.bfloat16
F32 = jnp.float32
MESH = pl.DeviceIdType.MESH


def dot(left, right):
    return jnp.dot(left, right, preferred_element_type=F32)


def kernel(
    panels,
    cols,
    pivot_rhs,
    update_rhs,
    parent_rhs,
    lower_pivot,
    lower_update,
    parent_lower,
    parent_upper,
    upper_pivot,
    upper_update,
    row_map,
    col_map,
    parent_out,
    child_out,
    pin,
    phalf,
    vec,
    x_pin,
    x_half,
    x_par,
    s_up,
    r_up,
    s_piv,
    r_piv,
    s_par,
    r_par,
    s_ch,
    r_ch,
    uhalf,
    moved,
    picked,
    direct,
    par_sum,
    spread_sum,
    child_sum,
    g_send,
    g_recv,
    f_send,
    rs_send,
    rs_recv,
    sh_send,
    sh_recv,
):
    me_p, me_r = lax.axis_index("panel"), lax.axis_index("rhs")
    total = panels * cols
    me = me_p * cols + me_r
    core = lax.rem(me_p, 2)
    mate = me_p + 1 - 2 * core
    per = panels // cols
    half = panels // 2
    m = parent_rhs.shape[0]
    mk = pivot_rhs.shape[1]
    child = me_p // half

    barrier = pltpu.get_barrier_semaphore()

    @pl.loop(1, total)
    def _(step):
        other = lax.rem(me + step, total)
        pl.semaphore_signal(
            barrier,
            inc=1,
            device_id=(other // cols, lax.rem(other, cols)),
            device_id_type=MESH,
        )

    pin[...] = pivot_rhs[...].astype(BF)
    direct[...] = jnp.zeros_like(direct)
    pl.semaphore_wait(barrier, total - 1)

    group = me_p // per
    last = cols - 1

    def every(source, goal):
        return None

    def below(source, goal):
        return goal >= source

    def above(source, goal):
        return goal <= source

    def guard(condition, action):
        if condition is None:
            action()
        else:
            pl.when(condition)(action)

    def both(first, second):
        return second if first is None else jnp.logical_and(first, second)

    def spot(buffer, depth, column, part, lead):
        rows = pl.ds(pl.multiple_of(part * depth, depth), depth)
        return buffer.at[column, slice(None) if lead is None else pl.ds(lead, 1), rows, :]

    class Gather:
        def __init__(self, stage, block, buffer, depth, keep, lead):
            self.stage, self.block, self.buffer, self.depth = stage, block, buffer, depth
            self.keep, self.lead = keep, lead
            self.active = keep(me_r, group)

        def place(self, column, part, panel):
            return spot(self.buffer, self.depth, column, part, self.lead(panel))

        def piece(self, panel):
            lead = self.lead(panel)
            return self.block if lead is None else self.block.at[pl.ds(lead, 1)]

        def goal(self, step):
            return lax.rem(me_p // 2 + step, half) * 2 + core

        def copy(self, step):
            goal = self.goal(step)
            return pltpu.make_async_remote_copy(
                src_ref=self.piece(goal),
                dst_ref=self.place(me_r, lax.rem(me_p, per), goal),
                send_sem=g_send.at[self.stage, step],
                recv_sem=g_recv.at[self.stage, me_r, lax.rem(me_p, per)],
                device_id=(goal, group),
                device_id_type=MESH,
            )

        def sends(self, action):
            for step in list(range(1, half)) + [0]:
                condition = self.keep(group, self.goal(step) // per)
                if step == 0:
                    condition = both(condition, group != me_r)
                guard(condition, functools.partial(action, step))

        def start(self):
            self.sends(lambda step: self.copy(step).start())

            @pl.when(group == me_r)
            def _():
                part = lax.rem(me_p, per)
                pltpu.make_async_copy(
                    self.piece(me_p),
                    self.place(me_r, part, me_p),
                    g_recv.at[self.stage, me_r, part],
                ).start()

        def landed(self, column, part):
            place = self.place(column, part, me_p)
            pltpu.make_async_copy(place, place, g_recv.at[self.stage, column, part]).wait()

        def forward(self, step, pair):
            column = lax.rem(me_r + 1 + step, cols)
            part = 2 * pair + core
            return pltpu.make_async_remote_copy(
                src_ref=self.place(column, part, me_p),
                dst_ref=self.place(column, part, me_p),
                send_sem=f_send.at[self.stage, step, pair],
                recv_sem=g_recv.at[self.stage, column, part],
                device_id=(mate, me_r),
                device_id_type=MESH,
            )

        def pass_on(self):
            def action():
                for step in [last] + list(range(last)):
                    for pair in range(per // 2):
                        self.landed(lax.rem(me_r + 1 + step, cols), 2 * pair + core)
                        self.forward(step, pair).start()

            guard(self.active, action)

        def arrive(self, step):
            column = lax.rem(me_r + 1 + step, cols)
            for pair in range(per // 2):
                self.landed(column, 2 * pair + 1 - core)
            return column

        def finish(self):
            self.sends(lambda step: self.copy(step).wait_send())

            def action():
                for step in range(cols):
                    for pair in range(per // 2):
                        self.forward(step, pair).wait_send()

            guard(self.active, action)

    class Scatter:
        def __init__(self, stage, source, target, keep):
            self.stage, self.source, self.target, self.keep = stage, source, target, keep
            self.active = keep(me_r, group)

        def copy(self, step):
            return pltpu.make_async_remote_copy(
                src_ref=self.source.at[step],
                dst_ref=self.target.at[step],
                send_sem=rs_send.at[self.stage, step],
                recv_sem=rs_recv.at[self.stage, step],
                device_id=(me_p, lax.rem(me_r + 1 + step, cols)),
                device_id_type=MESH,
            )

        def add(self, total_ref):
            for step in range(last):
                sender = lax.rem(me_r + last - step, cols)

                def action(step=step):
                    self.copy(step).wait_recv()
                    total_ref[...] += self.target[step].astype(F32)

                guard(self.keep(sender, group), action)

        def finish(self):
            def action():
                for step in range(last):
                    self.copy(step).wait_send()

            guard(self.active, action)

    def targets(ref, k, index, size, base):
        if ref.shape[0] == 2:
            return ref[k : k + 1, :]
        start = pl.multiple_of(k * (ref.shape[1] // 2) + index * size, 128)
        return ref[:, pl.ds(start, size)] - base

    def whole(panel):
        return None

    def same(panel):
        return panel // half

    def other(panel):
        return 1 - panel // half

    g_own = Gather(0, pin, x_pin, mk, every, same)
    g_other = Gather(5, pin, x_pin, mk, below, other)
    g_low = Gather(1, vec.at[0], x_par.at[0], m, below, whole)
    g_half = Gather(2, phalf, x_half, mk, above, whole)
    g_up = Gather(3, vec.at[1], x_par.at[1], m, above, whole)
    g_all = Gather(4, vec.at[2], x_par.at[2], m, every, whole)
    t_up = Scatter(0, s_up, r_up, every)
    t_piv = Scatter(1, s_piv, r_piv, below)
    t_low = Scatter(2, s_par.at[0], r_par.at[0], below)
    t_high = Scatter(3, s_par.at[1], r_par.at[1], above)
    t_child = Scatter(4, s_ch, r_ch, every)

    g_own.start()
    g_other.start()

    width = upper_update.shape[2]
    for k in range(2):
        rows = lax.broadcasted_iota(jnp.int32, (per * m, width), 0)
        chosen = (rows == targets(col_map, k, me_r, width, me_r * per * m)).astype(F32).astype(BF)
        picked[k] = lax.dot_general(
            upper_update[k], chosen, (((1,), (1,)), ((), ())), preferred_element_type=F32
        ).astype(BF)
    spread_sum[...] = parent_rhs[...]

    g_own.pass_on()
    for step in range(cols):
        column = g_own.arrive(step)
        value = dot(lower_update[...], x_pin[column, child])
        if step < last:
            s_up[step] = value.astype(BF)
            t_up.copy(step).start()
        else:
            par_sum[...] = update_rhs[...] + value
    g_other.pass_on()
    t_up.add(par_sum)
    update = par_sum[...].astype(BF)
    uhalf[0] = update[: m // 2]
    uhalf[1] = update[m // 2 :]
    first = lax.rem(me_p, half) * 2

    def shuffle(side):
        return pltpu.make_async_remote_copy(
            src_ref=uhalf.at[side],
            dst_ref=moved.at[child],
            send_sem=sh_send.at[side],
            recv_sem=sh_recv.at[child],
            device_id=(first + side, me_r),
            device_id_type=MESH,
        )

    for side in range(2):

        @pl.when(first + side != me_p)
        def _():
            shuffle(side).start()

        @pl.when(first + side == me_p)
        def _():
            pltpu.make_async_copy(uhalf.at[side], moved.at[child], sh_recv.at[child]).start()

    child_sum[...] = jnp.zeros_like(child_sum)

    def pivots():
        for step in range(cols):
            column = g_other.arrive(step)
            for k in range(2):
                value = dot(lower_pivot[k], x_pin[column, k])
                if step < last:
                    s_piv[step, k] = value.astype(BF)
                else:
                    child_sum[k] = value
            if step < last:
                t_piv.copy(step).start()

    guard(g_other.active, pivots)

    rows = lax.broadcasted_iota(jnp.int32, (m, m // 2), 0)
    for k in range(2):
        pltpu.make_async_copy(moved.at[k], moved.at[k], sh_recv.at[k]).wait()
        chosen = (rows == targets(row_map, k, me_p, m // 2, me_p * m)).astype(F32).astype(BF)
        spread_sum[...] += dot(chosen, moved[k])
    vec[0, 0] = spread_sum[...].astype(BF)
    g_low.start()

    t_piv.add(child_sum)
    phalf[...] = child_sum[...].astype(BF)
    g_half.start()

    def parent(level, gather, scatter, factor):
        par_sum[...] = jnp.zeros_like(par_sum)
        gather.pass_on()

        def action():
            for step in range(cols):
                column = gather.arrive(step)
                value = dot(factor[...], x_par[level, column, 0])
                if step < last:
                    s_par[level, step] = value.astype(BF)
                    scatter.copy(step).start()
                else:
                    par_sum[...] = value

        guard(gather.active, action)
        scatter.add(par_sum)
        vec[level + 1, 0] = par_sum[...].astype(BF)

    parent(0, g_low, t_low, parent_lower)
    g_up.start()
    g_half.pass_on()

    def known():
        for step in range(cols):
            column = g_half.arrive(step)
            for k in range(2):
                direct[step, k] = dot(upper_pivot[k], x_half[column, k])

    guard(g_half.active, known)
    parent(1, g_up, t_high, parent_upper)
    g_all.start()
    parent_out[...] = par_sum[...]

    g_all.pass_on()
    for step in range(cols):
        column = g_all.arrive(step)
        for k in range(2):
            value = direct[step, k] + dot(picked[k], x_par[2, column, 0])
            if step < last:
                s_ch[step, k] = value.astype(BF)
            else:
                child_out[k] = value
        if step < last:
            t_child.copy(step).start()
    for gather in (g_own, g_other, g_low, g_half, g_up, g_all):
        gather.finish()
    for side in range(2):

        @pl.when(first + side != me_p)
        def _():
            shuffle(side).wait_send()

    t_child.add(child_out)
    for scatter in (t_up, t_piv, t_low, t_high, t_child):
        scatter.finish()


def shards(panels, cols, *arguments):
    *arrays, maps = arguments
    m, width = arrays[1].shape
    mk = arrays[0].shape[1]
    per = panels // cols
    sides = maps.reshape(2, -1)
    me_p, me_r = lax.axis_index("panel"), lax.axis_index("rhs")
    wide = arrays[8].shape[2]

    def cut(index, size, base):
        if size % 128 == 0:
            return maps.reshape(1, -1)
        return lax.dynamic_slice_in_dim(sides, index * size, size, 1) - base

    row_map = cut(me_p, m // 2, me_p * m)
    col_map = cut(me_r, wide, me_r * per * m)
    vm = pltpu.VMEM
    dma = pltpu.SemaphoreType.DMA
    return pl.pallas_call(
        functools.partial(kernel, panels, cols),
        out_shape=(
            jax.ShapeDtypeStruct((m, width), F32),
            jax.ShapeDtypeStruct((2, mk, width), F32),
        ),
        in_specs=[pl.BlockSpec(memory_space=pltpu.VMEM)] * 11,
        out_specs=(pl.BlockSpec(memory_space=pltpu.VMEM),) * 2,
        scratch_shapes=[
            vm((2, mk, width), BF),
            vm((2, mk, width), BF),
            vm((3, 1, m, width), BF),
            vm((cols, 2, per * mk, width), BF),
            vm((cols, 2, per * mk, width), BF),
            vm((3, cols, 1, per * m, width), BF),
            vm((cols - 1, m, width), BF),
            vm((cols - 1, m, width), BF),
            vm((cols - 1, 2, mk, width), BF),
            vm((cols - 1, 2, mk, width), BF),
            vm((2, cols - 1, m, width), BF),
            vm((2, cols - 1, m, width), BF),
            vm((cols - 1, 2, mk, width), BF),
            vm((cols - 1, 2, mk, width), BF),
            vm((2, m // 2, width), BF),
            vm((2, m // 2, width), BF),
            vm((2, mk, per * m), BF),
            vm((cols, 2, mk, width), F32),
            vm((m, width), F32),
            vm((m, width), F32),
            vm((2, mk, width), F32),
            dma((6, panels // 2)),
            dma((6, cols, per)),
            dma((6, cols, per // 2)),
            dma((5, cols - 1)),
            dma((5, cols - 1)),
            dma((2,)),
            dma((2,)),
        ],
        compiler_params=pltpu.CompilerParams(
            collective_id=0, has_side_effects=True, vmem_limit_bytes=60 * 1024 * 1024
        ),
    )(*arrays, row_map, col_map)


def solution(mesh):
    panels, cols = mesh.shape["panel"], mesh.shape["rhs"]
    placed = (
        P(None, "panel", "rhs"),
        P("panel", "rhs"),
        P("panel", "rhs"),
        P(None, "panel", "rhs"),
        P("panel", "rhs"),
        P("panel", "rhs"),
        P("panel", "rhs"),
        P(None, "panel", "rhs"),
        P(None, "panel", "rhs"),
        P(),
    )
    return jax.shard_map(
        functools.partial(shards, panels, cols),
        mesh=mesh,
        in_specs=placed,
        out_specs=(P("panel", "rhs"), P(None, "panel", "rhs")),
        check_vma=False,
    )
```
